32 devices in a mesh: rep: 1 (over z), sub: 4 (over y), blk: 8 (over x, core).
Axes of the slice: x: 4, y: 4, z: 1, core: 2. Of those that a mesh axis runs over, the one named last changes fastest.
The devices are a block of a 4x4x8 slice.
Arguments:
- ratings: float32 [16384, 8192], P(('rep', 'blk', 'sub'))
- mask: int32 [16384, 8192], P(('rep', 'blk', 'sub'))
- user_init: float32 [16384, 256], P(('rep', 'blk', 'sub'))
- item_init: float32 [8192, 256], P(('rep', 'blk'))
Outputs:
- output 1: float32 [16384, 256], P(('rep', 'blk', 'sub'))
- output 2: float32 [8192, 256], P(('rep', 'blk'))
All inputs are finite; a program needn't handle non-finite values.
Results may differ from the reference program's by a relative error of at most 0.00127679.
Values are sent between devices in bfloat16 or wider.
A program may use at most 768 MiB of HBM per device.

```python
import math
import jax
import jax.numpy as jnp
from jax import lax

BLOCKS = 8
SUB_SHARDS = 4
USERS_DEV = 512
ITEMS_DEV = 1024
RANK = 256
STEPS = 4
EPOCHS = 2

USERS_BLK = SUB_SHARDS * USERS_DEV
USERS = BLOCKS * USERS_BLK
ITEMS = BLOCKS * ITEMS_DEV
BIG_SIDE = max(ITEMS_DEV, USERS_BLK)
STEP_SIZE = 0.4 * math.sqrt(RANK) / (math.sqrt(BIG_SIDE) + math.sqrt(RANK)) ** 2
WEIGHT_DECAY = 0.002 / STEP_SIZE


def setup_inputs(seed: int = 0, part: int = 0) -> dict:
    part_key = jax.random.fold_in(jax.random.key(seed), part)
    keys = jax.random.split(part_key, 7)
    user_true = jax.random.normal(keys[0], (USERS, RANK), jnp.float32)
    item_true = jax.random.normal(keys[1], (ITEMS, RANK), jnp.float32)
    noise = jax.random.normal(keys[2], (USERS, ITEMS), jnp.float32)
    ratings = jnp.dot(user_true, item_true.T) / math.sqrt(RANK) + 0.3 * noise
    block_pct = jax.random.randint(keys[3], (BLOCKS, 1, BLOCKS, 1), 10, 51)
    draws = jax.random.randint(keys[4], (BLOCKS, USERS_BLK, BLOCKS, ITEMS_DEV), 0, 100)
    mask = (draws < block_pct).astype(jnp.int32).reshape(USERS, ITEMS)
    init_scale = RANK ** -0.25
    user_init = jax.random.normal(keys[5], (USERS, RANK), jnp.float32) * init_scale
    item_init = jax.random.normal(keys[6], (ITEMS, RANK), jnp.float32) * init_scale
    return {'ratings': ratings, 'mask': mask, 'user_init': user_init, 'item_init': item_init}


def reference(ratings, mask, user_init, item_init):
    rating_blk = ratings.reshape(BLOCKS, USERS_BLK, BLOCKS, ITEMS_DEV)
    mask_blk = mask.reshape(BLOCKS, USERS_BLK, BLOCKS, ITEMS_DEV).astype(jnp.float32)
    block_ids = jnp.arange(BLOCKS)

    def sub_epoch(state, offset):
        cols = (block_ids + offset) % BLOCKS
        rating_now = rating_blk[block_ids, :, cols, :]
        mask_now = mask_blk[block_ids, :, cols, :]

        def grad_step(inner, unused):
            users, items = inner
            user_half = users.astype(jnp.bfloat16).astype(jnp.float32)
            item_half = items.astype(jnp.bfloat16).astype(jnp.float32)
            predicted = jnp.einsum('bur,bir->bui', user_half, item_half)
            err_half = (mask_now * (predicted - rating_now)).astype(jnp.bfloat16).astype(jnp.float32)
            grad_user = jnp.einsum('bui,bir->bur', err_half, item_half) + WEIGHT_DECAY * users
            grad_item = jnp.einsum('bui,bur->bir', err_half, user_half) + WEIGHT_DECAY * items
            return (users - STEP_SIZE * grad_user, items - STEP_SIZE * grad_item), None

        inner, unused = lax.scan(grad_step, state, None, length=STEPS)
        return (inner[0], jnp.roll(inner[1], -1, axis=0)), None

    start = (user_init.reshape(BLOCKS, USERS_BLK, RANK), item_init.reshape(BLOCKS, ITEMS_DEV, RANK))
    offsets = jnp.tile(block_ids, EPOCHS)
    final, unused = lax.scan(sub_epoch, start, offsets)
    return final[0].reshape(USERS, RANK), final[1].reshape(ITEMS, RANK)
```

```python
import functools
import math
import jax
import jax.numpy as jnp
from jax import lax
from jax.experimental import pallas as pl
from jax.experimental.pallas import tpu as pltpu
from jax.sharding import PartitionSpec as P

STEPS = 4
EPOCHS = 2
STEP_GAIN = 0.4
DECAY = 0.002
ITEM_CHUNK = 256
USER_CHUNK = 512
F32 = jnp.float32
BF16 = jnp.bfloat16


def kernel(n_sub, n_blk, step_size, decay_coef, ratings, mask, user_in, item_in, user_out, item_out, far_ratings,
           rating_buf, mask_buf, item_st, user_st, user_half, item_half, err_buf,
           own_sem, mask_sem, part_sem, rating_recv, rating_send, fwd_send, user_recv, user_send, item_recv, item_send,
           out_recv, out_send, last_recv, last_send):
    rep, sub, blk = lax.axis_index('rep'), lax.axis_index('sub'), lax.axis_index('blk')
    n = user_in.shape[0]
    half = n // 2
    n_chunks, factor_dim, width = item_in.shape
    items = n_chunks * width
    users = user_st.shape[0]
    n_turns = EPOCHS * n_blk

    def root_of(b):
        return (b // 2 + b) % 2 * (n_sub // 2)

    root = root_of(blk)
    rel = (sub + n_sub - root) % n_sub
    next_blk, prev_blk = (blk + n_blk - 1) % n_blk, (blk + 1) % n_blk
    far = (root + 2) % n_sub
    side = rel // 2

    def remote(src, dst, send_sem, recv_sem, to_sub, to_blk):
        return pltpu.make_async_remote_copy(src_ref=src, dst_ref=dst, send_sem=send_sem, recv_sem=recv_sem,
                                            device_id=(rep, to_sub, to_blk), device_id_type=pl.DeviceIdType.MESH)

    def arrived(dst, recv_sem):
        remote(dst, dst, user_send.at[0], recv_sem, (sub + 1) % n_sub, blk).wait_recv()

    barrier = pltpu.get_barrier_semaphore()
    for d in range(1, n_sub):
        pl.semaphore_signal(barrier, inc=1, device_id=(rep, (sub + d) % n_sub, blk), device_id_type=pl.DeviceIdType.MESH)

    @pl.when(rel == 0)
    def _():
        for b in (next_blk, prev_blk):
            pl.semaphore_signal(barrier, inc=1, device_id=(rep, root_of(b), b), device_id_type=pl.DeviceIdType.MESH)
        pl.semaphore_wait(barrier, n_sub + 1)

    @pl.when(rel != 0)
    def _():
        pl.semaphore_wait(barrier, n_sub - 1)

    def own_copies(t, slot):
        cols = pl.ds(pl.multiple_of((blk + t) % n_blk * items, items), items)
        return (pltpu.make_async_copy(ratings.at[:, cols], rating_buf.at[slot, pl.ds(0, n)], own_sem.at[slot]),
                pltpu.make_async_copy(mask.at[:, cols], mask_buf.at[slot], mask_sem.at[slot]))

    def load_own(t, slot):
        for copy in own_copies(t, slot):
            copy.start()

    def merge_own(t, slot, start):
        for copy in own_copies(t, slot):
            copy.wait()
        rating_buf[slot, pl.ds(start, n)] = jnp.where(mask_buf[slot] != 0, rating_buf[slot, pl.ds(0, n)], jnp.inf)

    def part_rows(k):
        return pl.ds((n, 2 * n, 3 * n, 3 * n + half)[k], (n, n, half, half)[k])

    def far_slice(t, rows):
        return far_ratings.at[t, pl.ds(rows.start - n, rows.size)]

    @pl.when(rel == 2)
    def _():
        load_own(0, 0)
        load_own(1, 1)
        first = [remote(user_in.at[pl.ds(k * half, half)], user_st.at[part_rows(2 + k)], user_send.at[k], user_recv.at[2 + k],
                        (root + 1 + 2 * k) % n_sub, blk) for k in range(2)]
        for copy in first:
            copy.start()

        def sends(t, slot):
            return [remote(rating_buf.at[slot, pl.ds(n + k * half, half)], far_slice(t, part_rows(2 + k)),
                           rating_send.at[slot, k], rating_recv.at[t, 2 + k], (root + 1 + 2 * k) % n_sub, blk) for k in range(2)]

        def turn(t, carry):
            slot = t % 2

            @pl.when(t >= 2)
            def _():
                for copy in sends(t - 2, slot):
                    copy.wait_send()
            merge_own(t, slot, n)
            for copy in sends(t, slot):
                copy.start()

            @pl.when(t + 2 < n_blk)
            def _():
                load_own(t + 2, slot)
            return carry

        lax.fori_loop(0, n_blk, turn, 0)
        for t in (n_blk - 2, n_blk - 1):
            for copy in sends(t, t % 2):
                copy.wait_send()
        for copy in first:
            copy.wait_send()
        for k in range(2):
            arrived(user_out.at[pl.ds(k * half, half)], out_recv.at[k])
        for c in range(n_chunks):
            arrived(item_out.at[c], last_recv.at[c])

    @pl.when((rel == 1) | (rel == 3))
    def _():
        load_own(0, 0)
        load_own(1, 1)
        own_start = pl.multiple_of(n + side * n, n)
        far_start = pl.multiple_of(3 * n + side * half, half)
        own_rows, far_rows = pl.ds(own_start, n), pl.ds(far_start, half)
        mine = remote(user_in, user_st.at[own_rows], user_send.at[0], user_recv.at[side], root, blk)
        mine.start()

        def own_send(t, slot):
            return remote(rating_buf.at[slot, pl.ds(n, n)], far_ratings.at[t, pl.ds(pl.multiple_of(own_start - n, n), n)],
                          rating_send.at[slot, 0], rating_recv.at[t, side], root, blk)

        def far_send(t, slot):
            there = far_ratings.at[t, pl.ds(pl.multiple_of(far_start - n, half), half)]
            return remote(there, there, fwd_send.at[slot], rating_recv.at[t, 2 + side], root, blk)

        arrived(user_st.at[far_rows], user_recv.at[2 + side])
        passed = remote(user_st.at[far_rows], user_st.at[far_rows], user_send.at[1], user_recv.at[2 + side], root, blk)
        passed.start()

        def turn(t, carry):
            slot = t % 2

            @pl.when(t >= 2)
            def _():
                own_send(t - 2, slot).wait_send()
                far_send(t - 2, slot).wait_send()
            merge_own(t, slot, n)
            own_send(t, slot).start()
            far_send(t, slot).wait_recv()
            far_send(t, slot).start()

            @pl.when(t + 2 < n_blk)
            def _():
                load_own(t + 2, slot)
            return carry

        lax.fori_loop(0, n_blk, turn, 0)
        for t in (n_blk - 2, n_blk - 1):
            own_send(t, t % 2).wait_send()
            far_send(t, t % 2).wait_send()
        mine.wait_send()
        passed.wait_send()
        arrived(user_st.at[pl.ds(0, half)], out_recv.at[2])
        back = remote(user_st.at[pl.ds(0, half)], user_out.at[pl.ds(pl.multiple_of(side * half, half), half)], out_send.at[0], out_recv.at[side], far, blk)
        back.start()
        arrived(user_out, out_recv.at[0])
        back_items = []
        for c in range(n_chunks):
            arrived(item_out.at[c], last_recv.at[c])
            copy = remote(item_out.at[c], item_out.at[c], last_send.at[c], last_recv.at[c], far, blk)
            mine_to_pass = side == (2 * c) // n_chunks

            @pl.when(mine_to_pass)
            def _():
                copy.start()
            back_items.append((copy, mine_to_pass))
        for copy, mine_to_pass in back_items:
            @pl.when(mine_to_pass)
            def _():
                copy.wait_send()
        back.wait_send()

    @pl.when(rel == 0)
    def _():
        load_own(0, 0)
        for c in range(n_chunks):
            item_st[0, c] = item_in[c]
        user_st[pl.ds(0, n)] = user_in[...]
        for k in range(4):
            arrived(user_st.at[part_rows(k)], user_recv.at[k])
        user_half[...] = user_st[...].astype(BF16)

        def part_copy(t, slot):
            return pltpu.make_async_copy(far_ratings.at[t % n_blk], rating_buf.at[slot, pl.ds(n, users - n)], part_sem.at[slot])

        def item_copy(t, c):
            return remote(item_st.at[t, c], item_st.at[t + 1, c], item_send.at[c], item_recv.at[t + 1, c], root_of(next_blk), next_blk)

        def step(t, slot, first, last):
            for c in range(n_chunks):
                if first:
                    @pl.when(t > 0)
                    def _():
                        arrived(item_st.at[t, c], item_recv.at[t, c])
                cols = pl.ds(c * width, width)
                item_old = item_st[t, c]
                item_now = item_old.astype(BF16)
                item_half[:, cols] = item_now
                predicted = jnp.dot(user_half[...], item_now, preferred_element_type=F32)
                rating = rating_buf[slot, :, cols]
                err = jnp.where(rating == jnp.inf, 0.0, predicted - rating).astype(BF16)
                err_buf[:, cols] = err
                grad_item = lax.dot_general(user_half[...], err, (((0,), (0,)), ((), ())), preferred_element_type=F32)
                item_st[t, c] = item_old - step_size * (grad_item + decay_coef * item_old)
                if last:
                    item_copy(t, c).start()
            for i in range(users // USER_CHUNK):
                rows = pl.ds(i * USER_CHUNK, USER_CHUNK)
                grad_user = lax.dot_general(err_buf[rows, :], item_half[...], (((1,), (1,)), ((), ())), preferred_element_type=F32)
                user_old = user_st[rows, :]
                user_new = user_old - step_size * (grad_user + decay_coef * user_old)
                user_st[rows, :] = user_new
                user_half[rows, :] = user_new.astype(BF16)

        def turn(t, carry):
            slot = t % 2

            @pl.when(t < n_blk)
            def _():
                for k in range(4):
                    arrived(far_slice(t, part_rows(k)), rating_recv.at[t, k])
                part_copy(t, slot).start()
            merge_own(t, slot, 0)
            part_copy(t, slot).wait()

            @pl.when(t + 1 < n_turns)
            def _():
                load_own(t + 1, 1 - slot)

            @pl.when((t + 1 >= n_blk) & (t + 1 < n_turns))
            def _():
                part_copy(t + 1, 1 - slot).start()
            step(t, slot, True, False)

            def middle(_, c):
                step(t, slot, False, False)
                return c

            lax.fori_loop(0, STEPS - 2, middle, 0)

            @pl.when(t > 0)
            def _():
                for c in range(n_chunks):
                    item_copy(t - 1, c).wait_send()
            step(t, slot, False, True)
            return carry

        lax.fori_loop(0, n_turns, turn, 0)
        outs = []
        for k in range(2):
            to = (root + 1 + 2 * k) % n_sub
            outs.append(remote(user_st.at[part_rows(2 + k)], user_st.at[pl.ds(0, half)], out_send.at[k], out_recv.at[2], to, blk))
        for k in range(2):
            to = (root + 1 + 2 * k) % n_sub
            outs.append(remote(user_st.at[part_rows(k)], user_out, out_send.at[2 + k], out_recv.at[0], to, blk))
        for copy in outs:
            copy.start()
        user_out[...] = user_st[pl.ds(0, n)]
        for c in range(n_chunks):
            arrived(item_st.at[n_turns, c], item_recv.at[n_turns, c])
            for k in range(2):
                to = (root + 1 + 2 * k) % n_sub
                copy = remote(item_st.at[n_turns, c], item_out.at[c], last_send.at[c + k * n_chunks], last_recv.at[c], to, blk)
                copy.start()
                outs.append(copy)
            item_out[c] = item_st[n_turns, c]
        for c in range(n_chunks):
            item_copy(n_turns - 1, c).wait_send()
        for copy in outs:
            copy.wait_send()


def solution(mesh):
    n_sub, n_blk = mesh.shape['sub'], mesh.shape['blk']
    row_spec = P(('rep', 'blk', 'sub'), None)
    item_spec = P(('rep', 'blk'), None)

    def local_run(ratings, mask, user_init, item_init):
        users_dev = ratings.shape[0]
        items_dev, factor_dim = item_init.shape
        users = n_sub * users_dev
        big_side = max(items_dev, users)
        step_size = STEP_GAIN * math.sqrt(factor_dim) / (math.sqrt(big_side) + math.sqrt(factor_dim)) ** 2
        decay_coef = DECAY / step_size
        n_chunks = items_dev // ITEM_CHUNK
        n_turns = EPOCHS * n_blk
        item_parts = item_init.reshape(n_chunks, ITEM_CHUNK, factor_dim).transpose(0, 2, 1)
        hbm, vmem = pl.BlockSpec(memory_space=pltpu.HBM), pl.BlockSpec(memory_space=pltpu.VMEM)
        dma = pltpu.SemaphoreType.DMA
        user_out, item_out, _ = pl.pallas_call(
            functools.partial(kernel, n_sub, n_blk, step_size, decay_coef),
            out_shape=(jax.ShapeDtypeStruct(user_init.shape, F32), jax.ShapeDtypeStruct(item_parts.shape, F32),
                       jax.ShapeDtypeStruct((n_blk, users - users_dev, items_dev), F32)),
            in_specs=[hbm, hbm, vmem, vmem],
            out_specs=(vmem, vmem, hbm),
            scratch_shapes=[
                pltpu.VMEM((2, users, items_dev), F32),
                pltpu.VMEM((2, users_dev, items_dev), jnp.int32),
                pltpu.VMEM((n_turns + 1,) + item_parts.shape, F32),
                pltpu.VMEM((users, factor_dim), F32),
                pltpu.VMEM((users, factor_dim), BF16),
                pltpu.VMEM((factor_dim, items_dev), BF16),
                pltpu.VMEM((users, items_dev), BF16),
                dma((2,)), dma((2,)), dma((2,)), dma((n_blk, 4)), dma((2, 2)), dma((2,)), dma((4,)), dma((2,)),
                dma((n_turns + 1, n_chunks)), dma((n_chunks,)), dma((3,)), dma((4,)), dma((n_chunks,)), dma((2 * n_chunks,)),
            ],
            compiler_params=pltpu.CompilerParams(collective_id=0, has_side_effects=True, vmem_limit_bytes=62 * 2**20),
            name='dsgd',
        )(ratings, mask, user_init, item_parts)
        return user_out, item_out.transpose(0, 2, 1).reshape(items_dev, factor_dim)

    return jax.shard_map(local_run, mesh=mesh, in_specs=(row_spec, row_spec, row_spec, item_spec), out_specs=(row_spec, item_spec), check_vma=False)
```

```python
import functools
import math
import jax
import jax.numpy as jnp
from jax import lax
from jax.experimental import pallas as pl
from jax.experimental.pallas import tpu as pltpu
from jax.sharding import PartitionSpec as P

STEPS = 4
EPOCHS = 2
STEP_GAIN = 0.4
DECAY = 0.002
ITEM_CHUNK = 256
USER_CHUNK = 512
PARTS = 2
DEPTH = 4
LAG = 1
F32 = jnp.float32
BF16 = jnp.bfloat16


def kernel(n_sub, n_blk, step_size, decay_coef, ratings, mask, user_in, item_in, user_out, item_out, far_ratings,
           rating_buf, mask_buf, item_st, user_st, user_half, item_half, err_buf,
           own_sem, mask_sem, part_sem, rating_recv, far_recv, relay_recv, rating_send, fwd_send, relay_sem, user_recv, user_send, item_recv, item_send,
           out_recv, out_send, last_recv, last_send):
    rep, sub, blk = lax.axis_index('rep'), lax.axis_index('sub'), lax.axis_index('blk')
    n_dev = user_in.shape[0]
    n = n_dev // PARTS
    half = n // 2
    n_chunks, factor_dim, width = item_in.shape
    items = n_chunks * width
    users = user_st.shape[0]
    n_turns = EPOCHS * n_blk

    def root_of(b):
        return b // 2 % 2 + b % 2 * (n_sub // 2)

    root = root_of(blk)
    rel = (sub + n_sub - root) % n_sub
    next_blk, prev_blk = (blk + n_blk - 1) % n_blk, (blk + 1) % n_blk
    side = rel // 2
    col = blk // 2
    n_cols = n_blk // 2
    twin, twin_from = (col + 1) % n_cols, (col + n_cols - 1) % n_cols
    region = n + half
    hot = (side + col) % 2 == 1
    direct_hot, direct_cold = n, n + half // 2

    def side_sub(k):
        return (root + 1 + 2 * k) % n_sub

    def relay_of(k):
        return 2 * twin + (root + 2 * n_sub - twin % 2 - 1 - 2 * k) % n_sub // 2

    twin_blk = 2 * twin_from + (sub + n_sub - twin_from % 2) % n_sub // 2

    def remote(src, dst, send_sem, recv_sem, to_sub, to_blk):
        return pltpu.make_async_remote_copy(src_ref=src, dst_ref=dst, send_sem=send_sem, recv_sem=recv_sem,
                                            device_id=(rep, to_sub, to_blk), device_id_type=pl.DeviceIdType.MESH)

    def arrived(dst, recv_sem):
        remote(dst, dst, user_send.at[0], recv_sem, (sub + 1) % n_sub, blk).wait_recv()

    barrier = pltpu.get_barrier_semaphore()

    def greet(to_sub, to_blk):
        pl.semaphore_signal(barrier, inc=1, device_id=(rep, to_sub, to_blk), device_id_type=pl.DeviceIdType.MESH)

    for d in range(1, n_sub):
        greet((sub + d) % n_sub, blk)

    @pl.when(rel == 0)
    def _():
        for b in (next_blk, prev_blk):
            greet(root_of(b), b)
        for k in range(2):
            greet(root, relay_of(k))
        pl.semaphore_wait(barrier, n_sub + 3)

    @pl.when(rel == 2)
    def _():
        pl.semaphore_wait(barrier, n_sub - 1)

    @pl.when((rel == 1) | (rel == 3))
    def _():
        greet(root, relay_of(side))
        greet((sub + 1 + 2 * side) % n_sub, twin_blk)
        greet(sub, twin_blk)
        pl.semaphore_wait(barrier, n_sub + 2)

    def col_range(t):
        return pl.ds(pl.multiple_of((blk + t) % n_blk * items, items), items)

    def own_copies(t, slot):
        return (pltpu.make_async_copy(ratings.at[:, col_range(t)], rating_buf.at[slot, pl.ds(0, n_dev)], own_sem.at[slot]),
                pltpu.make_async_copy(mask.at[:, col_range(t)], mask_buf.at[slot], mask_sem.at[slot]))

    def load_own(t, slot):
        for copy in own_copies(t, slot):
            copy.start()

    def merge_own(t, slot):
        for copy in own_copies(t, slot):
            copy.wait()
        rating_buf[slot, pl.ds(0, n_dev)] = jnp.where(mask_buf[slot] != 0, rating_buf[slot, pl.ds(0, n_dev)], jnp.inf)

    def buf_rows(h, start, size):
        return rating_buf.at[h % 2, pl.ds(pl.multiple_of(h % DEPTH // 2 * 2 * n + start, half // 2), size)]

    def mask_rows(h):
        return mask_buf.at[h % 2, pl.ds(pl.multiple_of(h % DEPTH // 2 * n, n), n)]

    def part_copies(h):
        rows = pl.ds(pl.multiple_of(h % PARTS * n, n), n)
        return (pltpu.make_async_copy(ratings.at[rows, col_range(h // PARTS)], buf_rows(h, 0, n), own_sem.at[h % DEPTH]),
                pltpu.make_async_copy(mask.at[rows, col_range(h // PARTS)], mask_rows(h), mask_sem.at[h % DEPTH]))

    def load_part(h):
        for copy in part_copies(h):
            copy.start()

    def merge_part(h):
        for copy in part_copies(h):
            copy.wait()
        buf_rows(h, n, n)[...] = jnp.where(mask_rows(h)[...] != 0, buf_rows(h, 0, n)[...], jnp.inf)

    n_parts = n_blk * PARTS

    def side_rows(k, p):
        return pl.ds(n_dev + (2 * p + k) * region, n)

    def far_rows_of(k, p):
        return pl.ds(n_dev + (2 * p + k) * region + n, half)

    @pl.when(rel == 2)
    def _():
        for h in range(DEPTH):
            load_part(h)
        first = [remote(user_in.at[pl.ds(p * n + k * half, half)], user_st.at[far_rows_of(k, p)], user_send.at[k + 2 * p],
                        user_recv.at[2 + k, p], side_sub(k), blk) for p in range(PARTS) for k in range(2)]
        for copy in first:
            copy.start()

        def sends(h):
            return [remote(buf_rows(h, n + k * half, half), far_ratings.at[h, pl.ds(k * region + n, half)],
                           rating_send.at[h % DEPTH, k], far_recv.at[h], side_sub(k), blk) for k in range(2)]

        def turn(h, carry):
            @pl.when(h >= DEPTH)
            def _():
                for copy in sends(h - DEPTH):
                    copy.wait_send()
            merge_part(h)
            for copy in sends(h):
                copy.start()

            @pl.when(h + DEPTH < n_parts)
            def _():
                load_part(h + DEPTH)
            return carry

        lax.fori_loop(0, n_parts, turn, 0)
        for h in range(n_parts - DEPTH, n_parts):
            for copy in sends(h):
                copy.wait_send()
        for copy in first:
            copy.wait_send()
        for p in range(PARTS):
            for k in range(2):
                arrived(user_out.at[pl.ds(p * n + k * half, half)], out_recv.at[2 * p + k])
        for c in range(n_chunks):
            arrived(item_out.at[c], last_recv.at[c])

    def run_side(is_hot):
        for h in range(DEPTH):
            load_part(h)
        base = side * region

        def user_rows(p, start, size):
            return user_st.at[pl.ds(pl.multiple_of(n_dev + 2 * p * region + base + start, half), size)]

        mine = [remote(user_in.at[pl.ds(p * n, n)], user_rows(p, 0, n), user_send.at[p], user_recv.at[side, p], root, blk) for p in range(PARTS)]
        for copy in mine:
            copy.start()
        direct = direct_hot if is_hot else direct_cold
        passed_on = direct_cold if is_hot else direct_hot
        relay = relay_of(side)

        def rows(start, size):
            return pl.ds(pl.multiple_of(base + start, half // 2), size)

        def cuts(lo, hi):
            if lo < direct < hi:
                return [(lo, direct), (direct, hi)]
            return [(lo, hi)]

        def to_root_or_relay(src, h, lo, hi, sem):
            if hi <= direct:
                return remote(src, far_ratings.at[h, rows(lo, hi - lo)], sem, rating_recv.at[h], root, blk)
            return remote(src, far_ratings.at[n_parts + h, rows(lo, hi - lo)], sem, relay_recv.at[h], root, relay)

        def own_sends(h):
            return [to_root_or_relay(buf_rows(h, n + lo, hi - lo), h, lo, hi, rating_send.at[h % DEPTH, i])
                    for i, (lo, hi) in enumerate(cuts(0, n))]

        def far_sends(h):
            return [to_root_or_relay(far_ratings.at[h, rows(lo, hi - lo)], h, lo, hi, fwd_send.at[h % DEPTH, i])
                    for i, (lo, hi) in enumerate(cuts(n, region))]

        def relay_send(h):
            there = rows(passed_on, region - passed_on)
            return remote(far_ratings.at[n_parts + h, there], far_ratings.at[h, there], relay_sem.at[h % DEPTH], rating_recv.at[h], sub, twin_blk)

        def relay_turn(h):
            @pl.when(h >= DEPTH)
            def _():
                relay_send(h - DEPTH).wait_send()
            there = rows(passed_on, region - passed_on)
            arrived(far_ratings.at[n_parts + h, there], relay_recv.at[h])
            relay_send(h).start()

        passed = []
        for p in range(PARTS):
            arrived(user_rows(p, n, half), user_recv.at[2 + side, p])
            passed.append(remote(user_rows(p, n, half), user_rows(p, n, half), user_send.at[2 + p], user_recv.at[2 + side, p], root, blk))
            passed[-1].start()

        def turn(h, carry):
            @pl.when(h >= DEPTH)
            def _():
                for copy in own_sends(h - DEPTH) + far_sends(h - DEPTH):
                    copy.wait_send()
            merge_part(h)
            for copy in own_sends(h):
                copy.start()
            arrived(far_ratings.at[h, rows(n, half)], far_recv.at[h])
            for copy in far_sends(h):
                copy.start()

            @pl.when(h + DEPTH < n_parts)
            def _():
                load_part(h + DEPTH)

            @pl.when(h >= LAG)
            def _():
                relay_turn(h - LAG)
            return carry

        lax.fori_loop(0, n_parts, turn, 0)
        for h in range(n_parts - LAG, n_parts):
            relay_turn(h)
        for h in range(n_parts - DEPTH, n_parts):
            for copy in own_sends(h) + far_sends(h) + [relay_send(h)]:
                copy.wait_send()
        for copy in mine + passed:
            copy.wait_send()

    @pl.when(((rel == 1) | (rel == 3)) & hot)
    def _():
        run_side(True)

    @pl.when(((rel == 1) | (rel == 3)) & jnp.logical_not(hot))
    def _():
        run_side(False)

    @pl.when((rel == 1) | (rel == 3))
    def _():
        far = (root + 2) % n_sub
        backs = []
        for p in range(PARTS):
            arrived(user_st.at[pl.ds(p * half, half)], out_recv.at[2 + p])
            backs.append(remote(user_st.at[pl.ds(p * half, half)], user_out.at[pl.ds(pl.multiple_of(p * n + side * half, half), half)],
                                out_send.at[p], out_recv.at[2 * p + side], far, blk))
            backs[-1].start()
        for p in range(PARTS):
            arrived(user_out.at[pl.ds(p * n, n)], out_recv.at[p])
        back_items = []
        for c in range(n_chunks):
            arrived(item_out.at[c], last_recv.at[c])
            copy = remote(item_out.at[c], item_out.at[c], last_send.at[c], last_recv.at[c], far, blk)
            mine_to_pass = side == (2 * c) // n_chunks

            @pl.when(mine_to_pass)
            def _():
                copy.start()
            back_items.append((copy, mine_to_pass))
        for copy, mine_to_pass in back_items:
            @pl.when(mine_to_pass)
            def _():
                copy.wait_send()
        for copy in backs:
            copy.wait_send()

    @pl.when(rel == 0)
    def _():
        load_own(0, 0)
        for c in range(n_chunks):
            item_st[0, c] = item_in[c]
        user_st[pl.ds(0, n_dev)] = user_in[...]
        for k in range(2):
            for p in range(PARTS):
                arrived(user_st.at[side_rows(k, p)], user_recv.at[k, p])
                arrived(user_st.at[far_rows_of(k, p)], user_recv.at[2 + k, p])
        user_half[...] = user_st[...].astype(BF16)

        def root_copies(t, slot):
            return [pltpu.make_async_copy(far_ratings.at[t % n_blk * PARTS + p], rating_buf.at[slot, pl.ds(n_dev + 2 * p * region, 2 * region)],
                                          part_sem.at[slot, p]) for p in range(PARTS)]

        def item_copy(t, c):
            return remote(item_st.at[t, c], item_st.at[t + 1, c], item_send.at[c], item_recv.at[t + 1, c], root_of(next_blk), next_blk)

        def step(t, slot, first, last):
            for c in range(n_chunks):
                if first:
                    @pl.when(t > 0)
                    def _():
                        arrived(item_st.at[t, c], item_recv.at[t, c])
                cols = pl.ds(c * width, width)
                item_old = item_st[t, c]
                item_now = item_old.astype(BF16)
                item_half[:, cols] = item_now
                predicted = jnp.dot(user_half[...], item_now, preferred_element_type=F32)
                rating = rating_buf[slot, :, cols]
                err = jnp.where(rating == jnp.inf, 0.0, predicted - rating).astype(BF16)
                err_buf[:, cols] = err
                grad_item = lax.dot_general(user_half[...], err, (((0,), (0,)), ((), ())), preferred_element_type=F32)
                item_st[t, c] = item_old - step_size * (grad_item + decay_coef * item_old)
                if last:
                    item_copy(t, c).start()
            for i in range(users // USER_CHUNK):
                rows = pl.ds(i * USER_CHUNK, USER_CHUNK)
                grad_user = lax.dot_general(err_buf[rows, :], item_half[...], (((1,), (1,)), ((), ())), preferred_element_type=F32)
                user_old = user_st[rows, :]
                user_new = user_old - step_size * (grad_user + decay_coef * user_old)
                user_st[rows, :] = user_new
                user_half[rows, :] = user_new.astype(BF16)

        def turn(t, carry):
            slot = t % 2

            @pl.when(t < n_blk)
            def _():
                for p, copy in enumerate(root_copies(t, slot)):
                    arrived(far_ratings.at[t * PARTS + p], rating_recv.at[t * PARTS + p])
                    copy.start()
            merge_own(t, slot)
            for copy in root_copies(t, slot):
                copy.wait()

            @pl.when(t + 1 < n_turns)
            def _():
                load_own(t + 1, 1 - slot)

            @pl.when((t + 1 >= n_blk) & (t + 1 < n_turns))
            def _():
                for copy in root_copies(t + 1, 1 - slot):
                    copy.start()
            step(t, slot, True, False)

            def middle(_, c):
                step(t, slot, False, False)
                return c

            lax.fori_loop(0, STEPS - 2, middle, 0)

            @pl.when(t > 0)
            def _():
                for c in range(n_chunks):
                    item_copy(t - 1, c).wait_send()
            step(t, slot, False, True)
            return carry

        lax.fori_loop(0, n_turns, turn, 0)
        outs = []
        for p in range(PARTS):
            for k in range(2):
                outs.append(remote(user_st.at[far_rows_of(k, p)], user_st.at[pl.ds(p * half, half)], out_send.at[2 * p + k], out_recv.at[2 + p], side_sub(k), blk))
        for p in range(PARTS):
            for k in range(2):
                outs.append(remote(user_st.at[side_rows(k, p)], user_out.at[pl.ds(p * n, n)], out_send.at[4 + 2 * p + k], out_recv.at[p], side_sub(k), blk))
        for copy in outs:
            copy.start()
        user_out[...] = user_st[pl.ds(0, n_dev)]
        for c in range(n_chunks):
            arrived(item_st.at[n_turns, c], item_recv.at[n_turns, c])
            for k in range(2):
                copy = remote(item_st.at[n_turns, c], item_out.at[c], last_send.at[c + k * n_chunks], last_recv.at[c], side_sub(k), blk)
                copy.start()
                outs.append(copy)
            item_out[c] = item_st[n_turns, c]
        for c in range(n_chunks):
            item_copy(n_turns - 1, c).wait_send()
        for copy in outs:
            copy.wait_send()


def solution(mesh):
    n_sub, n_blk = mesh.shape['sub'], mesh.shape['blk']
    row_spec = P(('rep', 'blk', 'sub'), None)
    item_spec = P(('rep', 'blk'), None)

    def local_run(ratings, mask, user_init, item_init):
        users_dev = ratings.shape[0]
        items_dev, factor_dim = item_init.shape
        users = n_sub * users_dev
        big_side = max(items_dev, users)
        step_size = STEP_GAIN * math.sqrt(factor_dim) / (math.sqrt(big_side) + math.sqrt(factor_dim)) ** 2
        decay_coef = DECAY / step_size
        n_chunks = items_dev // ITEM_CHUNK
        n_turns = EPOCHS * n_blk
        item_parts = item_init.reshape(n_chunks, ITEM_CHUNK, factor_dim).transpose(0, 2, 1)
        hbm, vmem = pl.BlockSpec(memory_space=pltpu.HBM), pl.BlockSpec(memory_space=pltpu.VMEM)
        dma = pltpu.SemaphoreType.DMA
        user_out, item_out, _ = pl.pallas_call(
            functools.partial(kernel, n_sub, n_blk, step_size, decay_coef),
            out_shape=(jax.ShapeDtypeStruct(user_init.shape, F32), jax.ShapeDtypeStruct(item_parts.shape, F32),
                       jax.ShapeDtypeStruct((2 * n_blk * PARTS, (users - users_dev) // PARTS, items_dev), F32)),
            in_specs=[hbm, hbm, vmem, vmem],
            out_specs=(vmem, vmem, hbm),
            scratch_shapes=[
                pltpu.VMEM((2, users, items_dev), F32),
                pltpu.VMEM((2, users_dev, items_dev), jnp.int32),
                pltpu.VMEM((n_turns + 1,) + item_parts.shape, F32),
                pltpu.VMEM((users, factor_dim), F32),
                pltpu.VMEM((users, factor_dim), BF16),
                pltpu.VMEM((factor_dim, items_dev), BF16),
                pltpu.VMEM((users, items_dev), BF16),
                dma((DEPTH,)), dma((DEPTH,)), dma((2, PARTS)), dma((n_blk * PARTS,)), dma((n_blk * PARTS,)), dma((n_blk * PARTS,)), dma((DEPTH, 2)), dma((DEPTH, 2)), dma((DEPTH,)),
                dma((4, PARTS)), dma((2 * PARTS,)),
                dma((n_turns + 1, n_chunks)), dma((n_chunks,)), dma((2 * PARTS,)), dma((4 * PARTS,)), dma((n_chunks,)), dma((2 * n_chunks,)),
            ],
            compiler_params=pltpu.CompilerParams(collective_id=0, has_side_effects=True, vmem_limit_bytes=62 * 2**20),
            name='dsgd',
        )(ratings, mask, user_init, item_parts)
        return user_out, item_out.transpose(0, 2, 1).reshape(items_dev, factor_dim)

    return jax.shard_map(local_run, mesh=mesh, in_specs=(row_spec, row_spec, row_spec, item_spec), out_specs=(row_spec, item_spec), check_vma=False)
```

```python
import functools
import math
import jax
import jax.numpy as jnp
from jax import lax
from jax.experimental import pallas as pl
from jax.experimental.pallas import tpu as pltpu
from jax.sharding import PartitionSpec as P

STEPS = 4
EPOCHS = 2
STEP_GAIN = 0.4
DECAY = 0.002
ITEM_CHUNK = 256
USER_CHUNK = 512
PARTS = 2
DEPTH = 4
LAG = 1
PIECES = 4
F32 = jnp.float32
BF16 = jnp.bfloat16


def kernel(n_sub, n_blk, step_size, decay_coef, ratings, mask, user_in, item_in, user_out, item_out, far_ratings,
           rating_buf, mask_buf, item_st, user_st, user_half, item_half, err_buf,
           own_sem, mask_sem, part_sem, rating_recv, far_recv, relay_recv, rating_send, fwd_send, relay_sem, user_recv, user_send, item_recv, item_send, hop_recv, hop_send,
           out_recv, out_send, last_recv, last_send):
    rep, sub, blk = lax.axis_index('rep'), lax.axis_index('sub'), lax.axis_index('blk')
    n_dev = user_in.shape[0]
    n = n_dev // PARTS
    half = n // 2
    n_chunks, factor_dim, width = item_in.shape
    items = n_chunks * width
    users = user_st.shape[0]
    n_turns = EPOCHS * n_blk

    def root_of(b):
        return b // 2 % 2 + b % 2 * (n_sub // 2)

    root = root_of(blk)
    rel = (sub + n_sub - root) % n_sub
    next_blk, prev_blk = (blk + n_blk - 1) % n_blk, (blk + 1) % n_blk
    side = rel // 2
    col = blk // 2
    n_cols = n_blk // 2
    twin, twin_from = (col + 1) % n_cols, (col + n_cols - 1) % n_cols
    region = n + half
    hot = (side + col) % 2 == 1
    direct_hot, direct_cold = n, n + half // 2

    def side_sub(k):
        return (root + 1 + 2 * k) % n_sub

    def relay_of(k):
        return 2 * twin + (root + 2 * n_sub - twin % 2 - 1 - 2 * k) % n_sub // 2

    twin_blk = 2 * twin_from + (sub + n_sub - twin_from % 2) % n_sub // 2

    def remote(src, dst, send_sem, recv_sem, to_sub, to_blk):
        return pltpu.make_async_remote_copy(src_ref=src, dst_ref=dst, send_sem=send_sem, recv_sem=recv_sem,
                                            device_id=(rep, to_sub, to_blk), device_id_type=pl.DeviceIdType.MESH)

    def arrived(dst, recv_sem):
        remote(dst, dst, user_send.at[0], recv_sem, (sub + 1) % n_sub, blk).wait_recv()

    barrier = pltpu.get_barrier_semaphore()

    def greet(to_sub, to_blk):
        pl.semaphore_signal(barrier, inc=1, device_id=(rep, to_sub, to_blk), device_id_type=pl.DeviceIdType.MESH)

    for d in range(1, n_sub):
        greet((sub + d) % n_sub, blk)

    @pl.when(rel == 0)
    def _():
        for b in (next_blk, prev_blk):
            greet(root_of(b), b)
        for k in range(2):
            greet(root, relay_of(k))
        relay_side = 1 - prev_blk // 2 % 2
        greet((root_of(prev_blk) + 1 + 2 * relay_side) % n_sub, prev_blk)
        pl.semaphore_wait(barrier, n_sub + 4)

    @pl.when(rel == 2)
    def _():
        pl.semaphore_wait(barrier, n_sub - 1)

    @pl.when((rel == 1) | (rel == 3))
    def _():
        greet(root, relay_of(side))
        greet((sub + 1 + 2 * side) % n_sub, twin_blk)
        greet(sub, twin_blk)

        @pl.when(hot)
        def _():
            greet(root_of(next_blk), next_blk)
            pl.semaphore_wait(barrier, n_sub + 3)

        @pl.when(jnp.logical_not(hot))
        def _():
            pl.semaphore_wait(barrier, n_sub + 2)

    def col_range(t):
        return pl.ds(pl.multiple_of((blk + t) % n_blk * items, items), items)

    def own_copies(t, slot):
        return (pltpu.make_async_copy(ratings.at[:, col_range(t)], rating_buf.at[slot, pl.ds(0, n_dev)], own_sem.at[slot]),
                pltpu.make_async_copy(mask.at[:, col_range(t)], mask_buf.at[slot], mask_sem.at[slot]))

    def load_own(t, slot):
        for copy in own_copies(t, slot):
            copy.start()

    def merge_own(t, slot):
        for copy in own_copies(t, slot):
            copy.wait()
        rating_buf[slot, pl.ds(0, n_dev)] = jnp.where(mask_buf[slot] != 0, rating_buf[slot, pl.ds(0, n_dev)], jnp.inf)

    def buf_rows(h, start, size):
        return rating_buf.at[h % 2, pl.ds(pl.multiple_of(h % DEPTH // 2 * 2 * n + start, half // 2), size)]

    def mask_rows(h):
        return mask_buf.at[h % 2, pl.ds(pl.multiple_of(h % DEPTH // 2 * n, n), n)]

    def part_copies(h):
        rows = pl.ds(pl.multiple_of(h % PARTS * n, n), n)
        return (pltpu.make_async_copy(ratings.at[rows, col_range(h // PARTS)], buf_rows(h, 0, n), own_sem.at[h % DEPTH]),
                pltpu.make_async_copy(mask.at[rows, col_range(h // PARTS)], mask_rows(h), mask_sem.at[h % DEPTH]))

    def load_part(h):
        for copy in part_copies(h):
            copy.start()

    def merge_part(h):
        for copy in part_copies(h):
            copy.wait()
        buf_rows(h, n, n)[...] = jnp.where(mask_rows(h)[...] != 0, buf_rows(h, 0, n)[...], jnp.inf)

    n_parts = n_blk * PARTS
    piece_rows = factor_dim // PIECES

    def side_rows(k, p):
        return pl.ds(n_dev + (2 * p + k) * region, n)

    def far_rows_of(k, p):
        return pl.ds(n_dev + (2 * p + k) * region + n, half)

    @pl.when(rel == 2)
    def _():
        for h in range(DEPTH):
            load_part(h)
        first = [remote(user_in.at[pl.ds(p * n + k * half, half)], user_st.at[far_rows_of(k, p)], user_send.at[k + 2 * p],
                        user_recv.at[2 + k, p], side_sub(k), blk) for p in range(PARTS) for k in range(2)]
        for copy in first:
            copy.start()

        def sends(h):
            return [remote(buf_rows(h, n + k * half, half), far_ratings.at[h, pl.ds(k * region + n, half)],
                           rating_send.at[h % DEPTH, k], far_recv.at[h], side_sub(k), blk) for k in range(2)]

        def turn(h, carry):
            @pl.when(h >= DEPTH)
            def _():
                for copy in sends(h - DEPTH):
                    copy.wait_send()
            merge_part(h)
            for copy in sends(h):
                copy.start()

            @pl.when(h + DEPTH < n_parts)
            def _():
                load_part(h + DEPTH)
            return carry

        lax.fori_loop(0, n_parts, turn, 0)
        for h in range(n_parts - DEPTH, n_parts):
            for copy in sends(h):
                copy.wait_send()
        for copy in first:
            copy.wait_send()
        for p in range(PARTS):
            for k in range(2):
                arrived(user_out.at[pl.ds(p * n + k * half, half)], out_recv.at[2 * p + k])
        for c in range(n_chunks):
            arrived(item_out.at[c], last_recv.at[c])

    def run_side(is_hot):
        for h in range(DEPTH):
            load_part(h)
        base = side * region

        def user_rows(p, start, size):
            return user_st.at[pl.ds(pl.multiple_of(n_dev + 2 * p * region + base + start, half), size)]

        mine = [remote(user_in.at[pl.ds(p * n, n)], user_rows(p, 0, n), user_send.at[p], user_recv.at[side, p], root, blk) for p in range(PARTS)]
        for copy in mine:
            copy.start()
        direct = direct_hot if is_hot else direct_cold
        passed_on = direct_cold if is_hot else direct_hot
        relay = relay_of(side)

        def rows(start, size):
            return pl.ds(pl.multiple_of(base + start, half // 2), size)

        def cuts(lo, hi):
            if lo < direct < hi:
                return [(lo, direct), (direct, hi)]
            return [(lo, hi)]

        def to_root_or_relay(src, h, lo, hi, sem):
            if hi <= direct:
                return remote(src, far_ratings.at[h, rows(lo, hi - lo)], sem, rating_recv.at[h], root, blk)
            return remote(src, far_ratings.at[n_parts + h, rows(lo, hi - lo)], sem, relay_recv.at[h], root, relay)

        def own_sends(h):
            return [to_root_or_relay(buf_rows(h, n + lo, hi - lo), h, lo, hi, rating_send.at[h % DEPTH, i])
                    for i, (lo, hi) in enumerate(cuts(0, n))]

        def far_sends(h):
            return [to_root_or_relay(far_ratings.at[h, rows(lo, hi - lo)], h, lo, hi, fwd_send.at[h % DEPTH, i])
                    for i, (lo, hi) in enumerate(cuts(n, region))]

        def relay_send(h):
            there = rows(passed_on, region - passed_on)
            return remote(far_ratings.at[n_parts + h, there], far_ratings.at[h, there], relay_sem.at[h % DEPTH], rating_recv.at[h], sub, twin_blk)

        def relay_turn(h):
            @pl.when(h >= DEPTH)
            def _():
                relay_send(h - DEPTH).wait_send()
            there = rows(passed_on, region - passed_on)
            arrived(far_ratings.at[n_parts + h, there], relay_recv.at[h])
            relay_send(h).start()

        passed = []
        for p in range(PARTS):
            arrived(user_rows(p, n, half), user_recv.at[2 + side, p])
            passed.append(remote(user_rows(p, n, half), user_rows(p, n, half), user_send.at[2 + p], user_recv.at[2 + side, p], root, blk))
            passed[-1].start()

        def turn(h, carry):
            @pl.when(h >= DEPTH)
            def _():
                for copy in own_sends(h - DEPTH) + far_sends(h - DEPTH):
                    copy.wait_send()
            merge_part(h)
            for copy in own_sends(h):
                copy.start()
            arrived(far_ratings.at[h, rows(n, half)], far_recv.at[h])
            for copy in far_sends(h):
                copy.start()

            @pl.when(h + DEPTH < n_parts)
            def _():
                load_part(h + DEPTH)

            @pl.when(h >= LAG)
            def _():
                relay_turn(h - LAG)
            return carry

        lax.fori_loop(0, n_parts, turn, 0)
        for h in range(n_parts - LAG, n_parts):
            relay_turn(h)
        for h in range(n_parts - DEPTH, n_parts):
            for copy in own_sends(h) + far_sends(h) + [relay_send(h)]:
                copy.wait_send()
        for copy in mine + passed:
            copy.wait_send()

    @pl.when(((rel == 1) | (rel == 3)) & hot)
    def _():
        run_side(True)

        def hop(t, i, q):
            piece = item_st.at[t + 1, 2 * i + 1, pl.ds(q * piece_rows, piece_rows)]
            return remote(piece, piece, hop_send.at[i, q], item_recv.at[t + 1, 2 * i + 1], root_of(next_blk), next_blk)

        def hops(t, carry):
            for i in range(n_chunks // 2):
                for q in range(PIECES):
                    @pl.when(t > n_blk)
                    def _():
                        hop(t - 1, i, q).wait_send()
                    arrived(item_st.at[t + 1, 2 * i + 1, pl.ds(q * piece_rows, piece_rows)], hop_recv.at[t - n_blk, i, q])
                    hop(t, i, q).start()
            return carry

        lax.fori_loop(n_blk, n_turns, hops, 0)
        for i in range(n_chunks // 2):
            for q in range(PIECES):
                hop(n_turns - 1, i, q).wait_send()

    @pl.when(((rel == 1) | (rel == 3)) & jnp.logical_not(hot))
    def _():
        run_side(False)

    @pl.when((rel == 1) | (rel == 3))
    def _():
        far = (root + 2) % n_sub
        backs = []
        for p in range(PARTS):
            arrived(user_st.at[pl.ds(p * half, half)], out_recv.at[2 + p])
            backs.append(remote(user_st.at[pl.ds(p * half, half)], user_out.at[pl.ds(pl.multiple_of(p * n + side * half, half), half)],
                                out_send.at[p], out_recv.at[2 * p + side], far, blk))
            backs[-1].start()
        for p in range(PARTS):
            arrived(user_out.at[pl.ds(p * n, n)], out_recv.at[p])
        back_items = []
        for c in range(n_chunks):
            arrived(item_out.at[c], last_recv.at[c])
            copy = remote(item_out.at[c], item_out.at[c], last_send.at[c], last_recv.at[c], far, blk)
            mine_to_pass = side == (2 * c) // n_chunks

            @pl.when(mine_to_pass)
            def _():
                copy.start()
            back_items.append((copy, mine_to_pass))
        for copy, mine_to_pass in back_items:
            @pl.when(mine_to_pass)
            def _():
                copy.wait_send()
        for copy in backs:
            copy.wait_send()

    @pl.when(rel == 0)
    def _():
        load_own(0, 0)
        for c in range(n_chunks):
            item_st[0, c] = item_in[c]
        user_st[pl.ds(0, n_dev)] = user_in[...]
        for k in range(2):
            for p in range(PARTS):
                arrived(user_st.at[side_rows(k, p)], user_recv.at[k, p])
                arrived(user_st.at[far_rows_of(k, p)], user_recv.at[2 + k, p])
        user_half[...] = user_st[...].astype(BF16)

        def root_copies(t, slot):
            return [pltpu.make_async_copy(far_ratings.at[t % n_blk * PARTS + p], rating_buf.at[slot, pl.ds(n_dev + 2 * p * region, 2 * region)],
                                          part_sem.at[slot, p]) for p in range(PARTS)]

        def item_copy(t, c):
            return remote(item_st.at[t, c], item_st.at[t + 1, c], item_send.at[c], item_recv.at[t + 1, c], root_of(next_blk), next_blk)

        def step(t, slot, first, last):
            for c in range(n_chunks):
                if first:
                    @pl.when(t > 0)
                    def _():
                        arrived(item_st.at[t, c], item_recv.at[t, c])
                cols = pl.ds(c * width, width)
                item_old = item_st[t, c]
                item_now = item_old.astype(BF16)
                item_half[:, cols] = item_now
                predicted = jnp.dot(user_half[...], item_now, preferred_element_type=F32)
                rating = rating_buf[slot, :, cols]
                err = jnp.where(rating == jnp.inf, 0.0, predicted - rating).astype(BF16)
                err_buf[:, cols] = err
                grad_item = lax.dot_general(user_half[...], err, (((0,), (0,)), ((), ())), preferred_element_type=F32)
                item_st[t, c] = item_old - step_size * (grad_item + decay_coef * item_old)
                if last and c % 2 == 0:
                    item_copy(t, c).start()
                if last and c % 2 == 1:
                    @pl.when(t < n_blk)
                    def _():
                        item_copy(t, c).start()

                    @pl.when(t >= n_blk)
                    def _():
                        for q in range(PIECES):
                            at = pl.ds(q * piece_rows, piece_rows)
                            remote(item_st.at[t, c, at], item_st.at[t + 1, c, at], item_send.at[c], hop_recv.at[t - n_blk, c // 2, q],
                                   side_sub(1 - col % 2), blk).start()
            for i in range(users // USER_CHUNK):
                rows = pl.ds(i * USER_CHUNK, USER_CHUNK)
                grad_user = lax.dot_general(err_buf[rows, :], item_half[...], (((1,), (1,)), ((), ())), preferred_element_type=F32)
                user_old = user_st[rows, :]
                user_new = user_old - step_size * (grad_user + decay_coef * user_old)
                user_st[rows, :] = user_new
                user_half[rows, :] = user_new.astype(BF16)

        def turn(t, carry):
            slot = t % 2

            @pl.when(t < n_blk)
            def _():
                for p, copy in enumerate(root_copies(t, slot)):
                    arrived(far_ratings.at[t * PARTS + p], rating_recv.at[t * PARTS + p])
                    copy.start()
            merge_own(t, slot)
            for copy in root_copies(t, slot):
                copy.wait()

            @pl.when(t + 1 < n_turns)
            def _():
                load_own(t + 1, 1 - slot)

            @pl.when((t + 1 >= n_blk) & (t + 1 < n_turns))
            def _():
                for copy in root_copies(t + 1, 1 - slot):
                    copy.start()
            step(t, slot, True, False)

            def middle(_, c):
                step(t, slot, False, False)
                return c

            lax.fori_loop(0, STEPS - 2, middle, 0)

            @pl.when(t > 0)
            def _():
                for c in range(n_chunks):
                    item_copy(t - 1, c).wait_send()
            step(t, slot, False, True)
            return carry

        lax.fori_loop(0, n_turns, turn, 0)
        outs = []
        for p in range(PARTS):
            for k in range(2):
                outs.append(remote(user_st.at[far_rows_of(k, p)], user_st.at[pl.ds(p * half, half)], out_send.at[2 * p + k], out_recv.at[2 + p], side_sub(k), blk))
        for p in range(PARTS):
            for k in range(2):
                outs.append(remote(user_st.at[side_rows(k, p)], user_out.at[pl.ds(p * n, n)], out_send.at[4 + 2 * p + k], out_recv.at[p], side_sub(k), blk))
        for copy in outs:
            copy.start()
        user_out[...] = user_st[pl.ds(0, n_dev)]
        for c in range(n_chunks):
            arrived(item_st.at[n_turns, c], item_recv.at[n_turns, c])
            for k in range(2):
                copy = remote(item_st.at[n_turns, c], item_out.at[c], last_send.at[c + k * n_chunks], last_recv.at[c], side_sub(k), blk)
                copy.start()
                outs.append(copy)
            item_out[c] = item_st[n_turns, c]
        for c in range(n_chunks):
            item_copy(n_turns - 1, c).wait_send()
        for copy in outs:
            copy.wait_send()


def solution(mesh):
    n_sub, n_blk = mesh.shape['sub'], mesh.shape['blk']
    row_spec = P(('rep', 'blk', 'sub'), None)
    item_spec = P(('rep', 'blk'), None)

    def local_run(ratings, mask, user_init, item_init):
        users_dev = ratings.shape[0]
        items_dev, factor_dim = item_init.shape
        users = n_sub * users_dev
        big_side = max(items_dev, users)
        step_size = STEP_GAIN * math.sqrt(factor_dim) / (math.sqrt(big_side) + math.sqrt(factor_dim)) ** 2
        decay_coef = DECAY / step_size
        n_chunks = items_dev // ITEM_CHUNK
        n_turns = EPOCHS * n_blk
        item_parts = item_init.reshape(n_chunks, ITEM_CHUNK, factor_dim).transpose(0, 2, 1)
        hbm, vmem = pl.BlockSpec(memory_space=pltpu.HBM), pl.BlockSpec(memory_space=pltpu.VMEM)
        dma = pltpu.SemaphoreType.DMA
        user_out, item_out, _ = pl.pallas_call(
            functools.partial(kernel, n_sub, n_blk, step_size, decay_coef),
            out_shape=(jax.ShapeDtypeStruct(user_init.shape, F32), jax.ShapeDtypeStruct(item_parts.shape, F32),
                       jax.ShapeDtypeStruct((2 * n_blk * PARTS, (users - users_dev) // PARTS, items_dev), F32)),
            in_specs=[hbm, hbm, vmem, vmem],
            out_specs=(vmem, vmem, hbm),
            scratch_shapes=[
                pltpu.VMEM((2, users, items_dev), F32),
                pltpu.VMEM((2, users_dev, items_dev), jnp.int32),
                pltpu.VMEM((n_turns + 1,) + item_parts.shape, F32),
                pltpu.VMEM((users, factor_dim), F32),
                pltpu.VMEM((users, factor_dim), BF16),
                pltpu.VMEM((factor_dim, items_dev), BF16),
                pltpu.VMEM((users, items_dev), BF16),
                dma((DEPTH,)), dma((DEPTH,)), dma((2, PARTS)), dma((n_blk * PARTS,)), dma((n_blk * PARTS,)), dma((n_blk * PARTS,)), dma((DEPTH, 2)), dma((DEPTH, 2)), dma((DEPTH,)),
                dma((4, PARTS)), dma((2 * PARTS,)),
                dma((n_turns + 1, n_chunks)), dma((n_chunks,)), dma((n_blk, n_chunks // 2, PIECES)), dma((n_chunks // 2, PIECES)), dma((2 * PARTS,)), dma((4 * PARTS,)), dma((n_chunks,)), dma((2 * n_chunks,)),
            ],
            compiler_params=pltpu.CompilerParams(collective_id=0, has_side_effects=True, vmem_limit_bytes=62 * 2**20),
            name='dsgd',
        )(ratings, mask, user_init, item_parts)
        return user_out, item_out.transpose(0, 2, 1).reshape(items_dev, factor_dim)

    return jax.shard_map(local_run, mesh=mesh, in_specs=(row_spec, row_spec, row_spec, item_spec), out_specs=(row_spec, item_spec), check_vma=False)
```

```python
import functools
import math
import jax
import jax.numpy as jnp
from jax import lax
from jax.experimental import pallas as pl
from jax.experimental.pallas import tpu as pltpu
from jax.sharding import PartitionSpec as P

STEPS = 4
EPOCHS = 2
STEP_GAIN = 0.4
DECAY = 0.002
ITEM_CHUNK = 256
USER_CHUNK = 512
PARTS = 2
DEPTH = 4
LAG = 1
PIECES = 8
F32 = jnp.float32
BF16 = jnp.bfloat16


def kernel(n_sub, n_blk, step_size, decay_coef, ratings, mask, user_in, item_in, user_out, item_out, far_ratings,
           rating_buf, mask_buf, item_st, user_st, user_half, item_half, err_buf,
           own_sem, mask_sem, part_sem, rating_recv, far_recv, relay_recv, rating_send, fwd_send, relay_sem, user_recv, user_send, item_recv, item_send, hop_recv, hop_send,
           out_recv, out_send, last_recv, last_send):
    rep, sub, blk = lax.axis_index('rep'), lax.axis_index('sub'), lax.axis_index('blk')
    n_dev = user_in.shape[0]
    n = n_dev // PARTS
    half = n // 2
    n_chunks, factor_dim, width = item_in.shape
    items = n_chunks * width
    users = user_st.shape[0]
    n_turns = EPOCHS * n_blk

    def root_of(b):
        return b // 2 % 2 + b % 2 * (n_sub // 2)

    root = root_of(blk)
    rel = (sub + n_sub - root) % n_sub
    next_blk, prev_blk = (blk + n_blk - 1) % n_blk, (blk + 1) % n_blk
    side = rel // 2
    col = blk // 2
    n_cols = n_blk // 2
    twin, twin_from = (col + 1) % n_cols, (col + n_cols - 1) % n_cols
    region = n + half
    hot = (side + col) % 2 == 1
    direct_hot, direct_cold = n, n + half // 2

    def side_sub(k):
        return (root + 1 + 2 * k) % n_sub

    def relay_of(k):
        return 2 * twin + (root + 2 * n_sub - twin % 2 - 1 - 2 * k) % n_sub // 2

    twin_blk = 2 * twin_from + (sub + n_sub - twin_from % 2) % n_sub // 2

    def remote(src, dst, send_sem, recv_sem, to_sub, to_blk):
        return pltpu.make_async_remote_copy(src_ref=src, dst_ref=dst, send_sem=send_sem, recv_sem=recv_sem,
                                            device_id=(rep, to_sub, to_blk), device_id_type=pl.DeviceIdType.MESH)

    def arrived(dst, recv_sem):
        remote(dst, dst, user_send.at[0], recv_sem, (sub + 1) % n_sub, blk).wait_recv()

    barrier = pltpu.get_barrier_semaphore()

    def greet(to_sub, to_blk):
        pl.semaphore_signal(barrier, inc=1, device_id=(rep, to_sub, to_blk), device_id_type=pl.DeviceIdType.MESH)

    for d in range(1, n_sub):
        greet((sub + d) % n_sub, blk)

    @pl.when(rel == 0)
    def _():
        for b in (next_blk, prev_blk):
            greet(root_of(b), b)
        for k in range(2):
            greet(root, relay_of(k))
        relay_side = 1 - prev_blk // 2 % 2
        greet((root_of(prev_blk) + 1 + 2 * relay_side) % n_sub, prev_blk)
        pl.semaphore_wait(barrier, n_sub + 4)

    @pl.when(rel == 2)
    def _():
        pl.semaphore_wait(barrier, n_sub - 1)

    @pl.when((rel == 1) | (rel == 3))
    def _():
        greet(root, relay_of(side))
        greet((sub + 1 + 2 * side) % n_sub, twin_blk)
        greet(sub, twin_blk)

        @pl.when(hot)
        def _():
            greet(root_of(next_blk), next_blk)
            pl.semaphore_wait(barrier, n_sub + 3)

        @pl.when(jnp.logical_not(hot))
        def _():
            pl.semaphore_wait(barrier, n_sub + 2)

    def col_range(t):
        return pl.ds(pl.multiple_of((blk + t) % n_blk * items, items), items)

    def own_copies(t, slot):
        return (pltpu.make_async_copy(ratings.at[:, col_range(t)], rating_buf.at[slot, pl.ds(0, n_dev)], own_sem.at[slot]),
                pltpu.make_async_copy(mask.at[:, col_range(t)], mask_buf.at[slot], mask_sem.at[slot]))

    def load_own(t, slot):
        for copy in own_copies(t, slot):
            copy.start()

    def merge_own(t, slot):
        for copy in own_copies(t, slot):
            copy.wait()
        rating_buf[slot, pl.ds(0, n_dev)] = jnp.where(mask_buf[slot] != 0, rating_buf[slot, pl.ds(0, n_dev)], jnp.inf)

    def buf_rows(h, start, size):
        return rating_buf.at[h % 2, pl.ds(pl.multiple_of(h % DEPTH // 2 * 2 * n + start, half // 2), size)]

    def mask_rows(h):
        return mask_buf.at[h % 2, pl.ds(pl.multiple_of(h % DEPTH // 2 * n, n), n)]

    def part_copies(h):
        rows = pl.ds(pl.multiple_of(h % PARTS * n, n), n)
        return (pltpu.make_async_copy(ratings.at[rows, col_range(h // PARTS)], buf_rows(h, 0, n), own_sem.at[h % DEPTH]),
                pltpu.make_async_copy(mask.at[rows, col_range(h // PARTS)], mask_rows(h), mask_sem.at[h % DEPTH]))

    def load_part(h):
        for copy in part_copies(h):
            copy.start()

    def merge_part(h):
        for copy in part_copies(h):
            copy.wait()
        buf_rows(h, n, n)[...] = jnp.where(mask_rows(h)[...] != 0, buf_rows(h, 0, n)[...], jnp.inf)

    n_parts = n_blk * PARTS
    piece_rows = factor_dim // PIECES

    def side_rows(k, p):
        return pl.ds(n_dev + (2 * p + k) * region, n)

    def far_rows_of(k, p):
        return pl.ds(n_dev + (2 * p + k) * region + n, half)

    @pl.when(rel == 2)
    def _():
        for h in range(DEPTH):
            load_part(h)
        first = [remote(user_in.at[pl.ds(p * n + k * half, half)], user_st.at[far_rows_of(k, p)], user_send.at[k + 2 * p],
                        user_recv.at[2 + k, p], side_sub(k), blk) for p in range(PARTS) for k in range(2)]
        for copy in first:
            copy.start()

        def sends(h):
            return [remote(buf_rows(h, n + k * half, half), far_ratings.at[h, pl.ds(k * region + n, half)],
                           rating_send.at[h % DEPTH, k], far_recv.at[h], side_sub(k), blk) for k in range(2)]

        def turn(h, carry):
            @pl.when(h >= DEPTH)
            def _():
                for copy in sends(h - DEPTH):
                    copy.wait_send()
            merge_part(h)
            for copy in sends(h):
                copy.start()

            @pl.when(h + DEPTH < n_parts)
            def _():
                load_part(h + DEPTH)
            return carry

        lax.fori_loop(0, n_parts, turn, 0)
        for h in range(n_parts - DEPTH, n_parts):
            for copy in sends(h):
                copy.wait_send()
        for copy in first:
            copy.wait_send()
        for p in range(PARTS):
            for k in range(2):
                arrived(user_out.at[pl.ds(p * n + k * half, half)], out_recv.at[2 * p + k])
        for c in range(n_chunks):
            arrived(item_out.at[c], last_recv.at[c])

    def run_side(is_hot):
        for h in range(DEPTH):
            load_part(h)
        base = side * region

        def user_rows(p, start, size):
            return user_st.at[pl.ds(pl.multiple_of(n_dev + 2 * p * region + base + start, half), size)]

        mine = [remote(user_in.at[pl.ds(p * n, n)], user_rows(p, 0, n), user_send.at[p], user_recv.at[side, p], root, blk) for p in range(PARTS)]
        for copy in mine:
            copy.start()
        direct = direct_hot if is_hot else direct_cold
        passed_on = direct_cold if is_hot else direct_hot
        relay = relay_of(side)

        def rows(start, size):
            return pl.ds(pl.multiple_of(base + start, half // 2), size)

        def cuts(lo, hi):
            if lo < direct < hi:
                return [(lo, direct), (direct, hi)]
            return [(lo, hi)]

        def to_root_or_relay(src, h, lo, hi, sem):
            if hi <= direct:
                return remote(src, far_ratings.at[h, rows(lo, hi - lo)], sem, rating_recv.at[h], root, blk)
            return remote(src, far_ratings.at[n_parts + h, rows(lo, hi - lo)], sem, relay_recv.at[h], root, relay)

        def own_sends(h):
            return [to_root_or_relay(buf_rows(h, n + lo, hi - lo), h, lo, hi, rating_send.at[h % DEPTH, i])
                    for i, (lo, hi) in enumerate(cuts(0, n))]

        def far_sends(h):
            return [to_root_or_relay(far_ratings.at[h, rows(lo, hi - lo)], h, lo, hi, fwd_send.at[h % DEPTH, i])
                    for i, (lo, hi) in enumerate(cuts(n, region))]

        def relay_send(h):
            there = rows(passed_on, region - passed_on)
            return remote(far_ratings.at[n_parts + h, there], far_ratings.at[h, there], relay_sem.at[h % DEPTH], rating_recv.at[h], sub, twin_blk)

        def relay_turn(h):
            @pl.when(h >= DEPTH)
            def _():
                relay_send(h - DEPTH).wait_send()
            there = rows(passed_on, region - passed_on)
            arrived(far_ratings.at[n_parts + h, there], relay_recv.at[h])
            relay_send(h).start()

        passed = []
        for p in range(PARTS):
            arrived(user_rows(p, n, half), user_recv.at[2 + side, p])
            passed.append(remote(user_rows(p, n, half), user_rows(p, n, half), user_send.at[2 + p], user_recv.at[2 + side, p], root, blk))
            passed[-1].start()

        def turn(h, carry):
            @pl.when(h >= DEPTH)
            def _():
                for copy in own_sends(h - DEPTH) + far_sends(h - DEPTH):
                    copy.wait_send()
            merge_part(h)
            for copy in own_sends(h):
                copy.start()
            arrived(far_ratings.at[h, rows(n, half)], far_recv.at[h])
            for copy in far_sends(h):
                copy.start()

            @pl.when(h + DEPTH < n_parts)
            def _():
                load_part(h + DEPTH)

            @pl.when(h >= LAG)
            def _():
                relay_turn(h - LAG)
            return carry

        lax.fori_loop(0, n_parts, turn, 0)
        for h in range(n_parts - LAG, n_parts):
            relay_turn(h)
        for h in range(n_parts - DEPTH, n_parts):
            for copy in own_sends(h) + far_sends(h) + [relay_send(h)]:
                copy.wait_send()
        for copy in mine + passed:
            copy.wait_send()

    @pl.when(((rel == 1) | (rel == 3)) & hot)
    def _():
        run_side(True)

        def hop(t, i, q):
            piece = item_st.at[t + 1, 2 * i + 1, pl.ds(q * piece_rows, piece_rows)]
            return remote(piece, piece, hop_send.at[i, q], item_recv.at[t + 1, 2 * i + 1], root_of(next_blk), next_blk)

        def hops(t, carry):
            for i in range(n_chunks // 2):
                for q in range(PIECES):
                    @pl.when(t > n_blk)
                    def _():
                        hop(t - 1, i, q).wait_send()
                    arrived(item_st.at[t + 1, 2 * i + 1, pl.ds(q * piece_rows, piece_rows)], hop_recv.at[t - n_blk, i, q])
                    hop(t, i, q).start()
            return carry

        lax.fori_loop(n_blk, n_turns, hops, 0)
        for i in range(n_chunks // 2):
            for q in range(PIECES):
                hop(n_turns - 1, i, q).wait_send()

    @pl.when(((rel == 1) | (rel == 3)) & jnp.logical_not(hot))
    def _():
        run_side(False)

    @pl.when((rel == 1) | (rel == 3))
    def _():
        far = (root + 2) % n_sub
        backs = []
        for p in range(PARTS):
            arrived(user_st.at[pl.ds(p * half, half)], out_recv.at[2 + p])
            backs.append(remote(user_st.at[pl.ds(p * half, half)], user_out.at[pl.ds(pl.multiple_of(p * n + side * half, half), half)],
                                out_send.at[p], out_recv.at[2 * p + side], far, blk))
            backs[-1].start()
        for p in range(PARTS):
            arrived(user_out.at[pl.ds(p * n, n)], out_recv.at[p])
        back_items = []
        for c in range(n_chunks):
            arrived(item_out.at[c], last_recv.at[c])
            copy = remote(item_out.at[c], item_out.at[c], last_send.at[c], last_recv.at[c], far, blk)
            mine_to_pass = side == (2 * c) // n_chunks

            @pl.when(mine_to_pass)
            def _():
                copy.start()
            back_items.append((copy, mine_to_pass))
        for copy, mine_to_pass in back_items:
            @pl.when(mine_to_pass)
            def _():
                copy.wait_send()
        for copy in backs:
            copy.wait_send()

    @pl.when(rel == 0)
    def _():
        load_own(0, 0)
        for c in range(n_chunks):
            item_st[0, c] = item_in[c]
        user_st[pl.ds(0, n_dev)] = user_in[...]
        for k in range(2):
            for p in range(PARTS):
                arrived(user_st.at[side_rows(k, p)], user_recv.at[k, p])
                arrived(user_st.at[far_rows_of(k, p)], user_recv.at[2 + k, p])
        user_half[...] = user_st[...].astype(BF16)

        def root_copies(t, slot):
            return [pltpu.make_async_copy(far_ratings.at[t % n_blk * PARTS + p], rating_buf.at[slot, pl.ds(n_dev + 2 * p * region, 2 * region)],
                                          part_sem.at[slot, p]) for p in range(PARTS)]

        def item_copy(t, c):
            return remote(item_st.at[t, c], item_st.at[t + 1, c], item_send.at[c], item_recv.at[t + 1, c], root_of(next_blk), next_blk)

        def step(t, slot, first, last):
            for c in range(n_chunks):
                if first:
                    @pl.when(t > 0)
                    def _():
                        arrived(item_st.at[t, c], item_recv.at[t, c])
                cols = pl.ds(c * width, width)
                item_old = item_st[t, c]
                item_now = item_old.astype(BF16)
                item_half[:, cols] = item_now
                predicted = jnp.dot(user_half[...], item_now, preferred_element_type=F32)
                rating = rating_buf[slot, :, cols]
                err = jnp.where(rating == jnp.inf, 0.0, predicted - rating).astype(BF16)
                err_buf[:, cols] = err
                grad_item = lax.dot_general(user_half[...], err, (((0,), (0,)), ((), ())), preferred_element_type=F32)
                item_st[t, c] = item_old - step_size * (grad_item + decay_coef * item_old)
                if last and c % 2 == 0:
                    item_copy(t, c).start()
                if last and c % 2 == 1:
                    @pl.when(t < n_blk)
                    def _():
                        item_copy(t, c).start()

                    @pl.when(t >= n_blk)
                    def _():
                        for q in range(PIECES):
                            at = pl.ds(q * piece_rows, piece_rows)
                            remote(item_st.at[t, c, at], item_st.at[t + 1, c, at], item_send.at[c], hop_recv.at[t - n_blk, c // 2, q],
                                   side_sub(1 - col % 2), blk).start()
            for i in range(users // USER_CHUNK):
                rows = pl.ds(i * USER_CHUNK, USER_CHUNK)
                grad_user = lax.dot_general(err_buf[rows, :], item_half[...], (((1,), (1,)), ((), ())), preferred_element_type=F32)
                user_old = user_st[rows, :]
                user_new = user_old - step_size * (grad_user + decay_coef * user_old)
                user_st[rows, :] = user_new
                user_half[rows, :] = user_new.astype(BF16)

        def turn(t, carry):
            slot = t % 2

            @pl.when(t < n_blk)
            def _():
                for p, copy in enumerate(root_copies(t, slot)):
                    arrived(far_ratings.at[t * PARTS + p], rating_recv.at[t * PARTS + p])
                    copy.start()
            merge_own(t, slot)
            for copy in root_copies(t, slot):
                copy.wait()

            @pl.when(t + 1 < n_turns)
            def _():
                load_own(t + 1, 1 - slot)

            @pl.when((t + 1 >= n_blk) & (t + 1 < n_turns))
            def _():
                for copy in root_copies(t + 1, 1 - slot):
                    copy.start()
            step(t, slot, True, False)

            def middle(_, c):
                step(t, slot, False, False)
                return c

            lax.fori_loop(0, STEPS - 2, middle, 0)

            @pl.when(t > 0)
            def _():
                for c in range(n_chunks):
                    item_copy(t - 1, c).wait_send()
            step(t, slot, False, True)
            return carry

        lax.fori_loop(0, n_turns, turn, 0)
        outs = []
        for p in range(PARTS):
            for k in range(2):
                outs.append(remote(user_st.at[far_rows_of(k, p)], user_st.at[pl.ds(p * half, half)], out_send.at[2 * p + k], out_recv.at[2 + p], side_sub(k), blk))
        for p in range(PARTS):
            for k in range(2):
                outs.append(remote(user_st.at[side_rows(k, p)], user_out.at[pl.ds(p * n, n)], out_send.at[4 + 2 * p + k], out_recv.at[p], side_sub(k), blk))
        for copy in outs:
            copy.start()
        user_out[...] = user_st[pl.ds(0, n_dev)]
        for c in range(n_chunks):
            arrived(item_st.at[n_turns, c], item_recv.at[n_turns, c])
            for k in range(2):
                copy = remote(item_st.at[n_turns, c], item_out.at[c], last_send.at[c + k * n_chunks], last_recv.at[c], side_sub(k), blk)
                copy.start()
                outs.append(copy)
            item_out[c] = item_st[n_turns, c]
        for c in range(n_chunks):
            item_copy(n_turns - 1, c).wait_send()
        for copy in outs:
            copy.wait_send()


def solution(mesh):
    n_sub, n_blk = mesh.shape['sub'], mesh.shape['blk']
    row_spec = P(('rep', 'blk', 'sub'), None)
    item_spec = P(('rep', 'blk'), None)

    def local_run(ratings, mask, user_init, item_init):
        users_dev = ratings.shape[0]
        items_dev, factor_dim = item_init.shape
        users = n_sub * users_dev
        big_side = max(items_dev, users)
        step_size = STEP_GAIN * math.sqrt(factor_dim) / (math.sqrt(big_side) + math.sqrt(factor_dim)) ** 2
        decay_coef = DECAY / step_size
        n_chunks = items_dev // ITEM_CHUNK
        n_turns = EPOCHS * n_blk
        item_parts = item_init.reshape(n_chunks, ITEM_CHUNK, factor_dim).transpose(0, 2, 1)
        hbm, vmem = pl.BlockSpec(memory_space=pltpu.HBM), pl.BlockSpec(memory_space=pltpu.VMEM)
        dma = pltpu.SemaphoreType.DMA
        user_out, item_out, _ = pl.pallas_call(
            functools.partial(kernel, n_sub, n_blk, step_size, decay_coef),
            out_shape=(jax.ShapeDtypeStruct(user_init.shape, F32), jax.ShapeDtypeStruct(item_parts.shape, F32),
                       jax.ShapeDtypeStruct((2 * n_blk * PARTS, (users - users_dev) // PARTS, items_dev), F32)),
            in_specs=[hbm, hbm, vmem, vmem],
            out_specs=(vmem, vmem, hbm),
            scratch_shapes=[
                pltpu.VMEM((2, users, items_dev), F32),
                pltpu.VMEM((2, users_dev, items_dev), jnp.int32),
                pltpu.VMEM((n_turns + 1,) + item_parts.shape, F32),
                pltpu.VMEM((users, factor_dim), F32),
                pltpu.VMEM((users, factor_dim), BF16),
                pltpu.VMEM((factor_dim, items_dev), BF16),
                pltpu.VMEM((users, items_dev), BF16),
                dma((DEPTH,)), dma((DEPTH,)), dma((2, PARTS)), dma((n_blk * PARTS,)), dma((n_blk * PARTS,)), dma((n_blk * PARTS,)), dma((DEPTH, 2)), dma((DEPTH, 2)), dma((DEPTH,)),
                dma((4, PARTS)), dma((2 * PARTS,)),
                dma((n_turns + 1, n_chunks)), dma((n_chunks,)), dma((n_blk, n_chunks // 2, PIECES)), dma((n_chunks // 2, PIECES)), dma((2 * PARTS,)), dma((4 * PARTS,)), dma((n_chunks,)), dma((2 * n_chunks,)),
            ],
            compiler_params=pltpu.CompilerParams(collective_id=0, has_side_effects=True, vmem_limit_bytes=62 * 2**20),
            name='dsgd',
        )(ratings, mask, user_init, item_parts)
        return user_out, item_out.transpose(0, 2, 1).reshape(items_dev, factor_dim)

    return jax.shard_map(local_run, mesh=mesh, in_specs=(row_spec, row_spec, row_spec, item_spec), out_specs=(row_spec, item_spec), check_vma=False)
```
